32 devices in a mesh: section: 2 (over y), row: 4 (over z), col: 4 (over x, core).
Axes of the slice: x: 2, y: 2, z: 4, core: 2. Of those that a mesh axis runs over, the one named last changes fastest.
Arguments:
- tokens: bfloat16 [2, 256, 6144], P(None, 'col', 'row'), may hold values from -6 to 6
- ln_gain: float32 [2, 6144], P('section', 'row'), may hold values from 0.1 to 1.9
- w_query: bfloat16 [2, 6144, 6144], P('section', 'row', 'col'), as said below
- w_key: bfloat16 [2, 6144, 6144], P('section', 'row', 'col'), as said below
- w_value: bfloat16 [2, 6144, 6144], P('section', 'row', 'col'), may hold values from -0.078125 to 0.078125
- w_up: bfloat16 [2, 6144, 24576], P('section', 'row', 'col'), may hold values from -0.078125 to 0.078125
- w_out: bfloat16 [2, 6144, 6144], P('section', 'col', 'row'), may hold values from -0.078125 to 0.078125
- w_down: bfloat16 [2, 24576, 6144], P('section', 'col', 'row'), may hold values from -0.0390625 to 0.0390625
Outputs:
- section_out: bfloat16 [2, 2, 256, 6144], P('section', None, 'col', 'row')
The draws below stay inside these ranges and needn't reach their ends.
Inputs may be any that keep to these rules, and one draw needn't show every extreme that they name: `w_query`: entries are normal with standard deviation 6144 ** -0.5, clipped at six deviations. `w_key`: entries are of the order of 6144 ** -0.5; in some heads the key columns may be up to twenty times larger and correlated with the query columns.
All inputs are finite; a program needn't handle non-finite values.
Results may differ from the reference program's by a relative error of at most 0.02.
Values may be sent and summed in bfloat16 or wider, within the bound.
A program may use at most 128 MiB of HBM per device.

```python
import jax
import jax.numpy as jnp
from jax import lax

D = 6144
HEADS = 48
MLP = 24576
PATCHES = 256
IMAGES = 2
LAYERS = 2
N_ROW = 4


def base_query(key):
    values = jax.random.normal(jax.random.fold_in(key, 101), (LAYERS, D, D), jnp.float32)
    return jnp.clip(values, -6.0, 6.0) * D ** (-0.5)


def draw_w_query(key, part):
    return base_query(key).astype(jnp.bfloat16)


def draw_w_key(key, part):
    fresh = jax.random.normal(jax.random.fold_in(key, 202), (LAYERS, D, D), jnp.float32)
    fresh = jnp.clip(fresh, -6.0, 6.0) * D ** (-0.5)
    return fresh.astype(jnp.bfloat16)


def level_of(key, dims, split, low, high):
    factor_of, own = 1.0, jax.random.fold_in(key, 6)
    for dim, parts in split:
        heights = jnp.exp(jax.random.uniform(jax.random.fold_in(own, dim), (parts,), jnp.float32, low / len(split), high / len(split)))
        factor_of = factor_of * jnp.repeat(heights, dims[dim] // parts).reshape([-1 if axis == dim else 1 for axis in range(len(dims))])
    return factor_of


def bell_draw(stream_key, extent, spread, reach, cuts=(), dtype=jnp.bfloat16):
    values = spread * jax.random.normal(stream_key, extent, jnp.float32)
    if cuts:
        values = values * level_of(stream_key, extent, cuts, -0.22, 0.18)
    return jnp.clip(values, -reach, reach).astype(dtype)


def setup_inputs(seed: int = 0) -> dict:
    keys = jax.random.split(jax.random.key(seed), 9)
    tokens = bell_draw(keys[0], (IMAGES, PATCHES, D), 1.0, 6.0, ((1, 4), (2, 4)))
    ln_gain = jnp.clip(1.0 + 0.18 * jax.random.normal(keys[1], (LAYERS, D), jnp.float32), 0.1, 1.9)
    w_query = draw_w_query(jax.random.fold_in(keys[8], 71), 0)
    w_key = draw_w_key(jax.random.fold_in(keys[8], 71), 0)
    w_value = bell_draw(keys[4], (LAYERS, D, D), D ** -0.5, 0.078125, ((0, 2), (1, 4), (2, 4)))
    w_up = bell_draw(keys[5], (LAYERS, D, MLP), D ** -0.5, 0.078125, ((0, 2), (1, 4), (2, 4)))
    w_out = bell_draw(keys[6], (LAYERS, D, D), D ** -0.5, 0.078125, ((0, 2), (1, 4), (2, 4)))
    w_down = bell_draw(keys[7], (LAYERS, MLP, D), MLP ** -0.5, 0.0390625, ((0, 2), (1, 4), (2, 4)))
    return dict(tokens=tokens, ln_gain=ln_gain, w_query=w_query, w_key=w_key, w_value=w_value, w_up=w_up, w_out=w_out, w_down=w_down)


EPS = 1e-06

def project(normed, weight):
    block_width = D // N_ROW
    total = jnp.zeros((normed.shape[0], normed.shape[1], weight.shape[1]), jnp.float32)
    for block in range(N_ROW):
        part = jnp.dot(normed[:, :, block * block_width:(block + 1) * block_width], weight[block * block_width:(block + 1) * block_width], preferred_element_type=jnp.float32)
        total = total + lax.optimization_barrier(part.astype(jnp.bfloat16)).astype(jnp.float32)
    return total

def layer(x, gain, wq, wk, wv, wup, wout, wdown):
    xf = x.astype(jnp.float32)
    mean = lax.optimization_barrier(jnp.mean(xf, axis=-1, keepdims=True))
    var = jnp.maximum(lax.optimization_barrier(jnp.mean(xf * xf, axis=-1, keepdims=True)) - mean * mean, 0.0)
    normed = ((xf - mean) * lax.rsqrt(var + EPS) * gain.astype(jnp.float32)).astype(jnp.bfloat16)
    query = project(normed, wq).astype(jnp.bfloat16)
    keyed = project(normed, wk).astype(jnp.bfloat16)
    valued = project(normed, wv).astype(jnp.bfloat16)
    act = jax.nn.gelu(project(normed, wup), approximate=False).astype(jnp.bfloat16)
    head_dim = D // HEADS
    shape = (x.shape[0], x.shape[1], HEADS, head_dim)
    qh = query.reshape(shape).astype(jnp.float32)
    kh = keyed.reshape(shape).astype(jnp.float32)
    vh = valued.reshape(shape).astype(jnp.float32)
    scores = jnp.einsum('bqhd,bkhd->bhqk', qh, kh) / jnp.sqrt(jnp.float32(head_dim))
    scores = scores - lax.optimization_barrier(jnp.max(scores, axis=-1, keepdims=True))
    weights = jnp.exp(scores)
    probs = (weights / lax.optimization_barrier(jnp.sum(weights, axis=-1, keepdims=True))).astype(jnp.bfloat16)
    attn = jnp.einsum('bhqk,bkhd->bqhd', probs.astype(jnp.float32), vh)
    attn = attn.reshape(x.shape).astype(jnp.bfloat16)
    mixed = jnp.dot(attn, wout, preferred_element_type=jnp.float32) + jnp.dot(act, wdown, preferred_element_type=jnp.float32)
    return (xf + mixed).astype(jnp.bfloat16)

def reference(tokens, ln_gain, w_query, w_key, w_value, w_up, w_out, w_down):
    current = tokens
    outputs = []
    for level in range(LAYERS):
        current = layer(current, ln_gain[level], w_query[level], w_key[level], w_value[level], w_up[level], w_out[level], w_down[level])
        outputs.append(current)
    return jnp.stack(outputs)
```

```python
import functools

import jax
import jax.numpy as jnp
from jax import lax
from jax.experimental import pallas as pl
from jax.experimental.pallas import tpu as pltpu
from jax.sharding import PartitionSpec as P

D = 6144
HEADS = 48


EPS = 1e-06
MESH = pl.DeviceIdType.MESH
PIECE = 16
SKEW = 3
VMEM_BYTES = 56 * 1024 * 1024


def params(collective_id):
    return pltpu.CompilerParams(
        collective_id=collective_id, has_side_effects=True, vmem_limit_bytes=VMEM_BYTES
    )


def vmem():
    return pl.BlockSpec(memory_space=pltpu.VMEM)


def greet_peers(axes):
    barrier = pltpu.get_barrier_semaphore()
    total = 0
    for axis, count in axes:
        me = lax.axis_index(axis)
        for step in range(1, count):
            pl.semaphore_signal(
                barrier, inc=1, device_id={axis: lax.rem(me + step, count)}, device_id_type=MESH
            )
            total += 1
    pl.semaphore_wait(barrier, total)


def greet_line(me, count):
    barrier = pltpu.get_barrier_semaphore()

    @pl.when(me > 0)
    def _():
        pl.semaphore_signal(barrier, inc=1, device_id={"row": me - 1}, device_id_type=MESH)

    @pl.when(me < count - 1)
    def _():
        pl.semaphore_signal(barrier, inc=1, device_id={"row": me + 1}, device_id_type=MESH)

    pl.semaphore_wait(barrier, jnp.where(jnp.logical_and(me > 0, me < count - 1), 2, 1))


def norm_kernel(rows, cols, x_ref, gain_ref, out_ref, mine, stats, stat_send, stat_recv, send, recv, local_sem):
    me_row, me_col = lax.axis_index("row"), lax.axis_index("col")
    patches, width = x_ref.shape
    greet_peers((("row", rows), ("col", cols)))
    xf = x_ref[...].astype(jnp.float32)
    total = jnp.sum(xf, axis=-1, keepdims=True)
    square = jnp.sum(xf * xf, axis=-1, keepdims=True)
    lane = lax.broadcasted_iota(jnp.int32, (patches, 128), 1)
    stats[0] = jnp.where(lane < 64, total, square)
    copies = []
    for step in range(1, rows):
        copy = pltpu.make_async_remote_copy(
            src_ref=stats.at[0],
            dst_ref=stats.at[step],
            send_sem=stat_send.at[step],
            recv_sem=stat_recv.at[step],
            device_id={"row": lax.rem(me_row + step, rows)},
            device_id_type=MESH,
        )
        copy.start()
        copies.append(copy)
    for copy in copies:
        copy.wait()
    both = stats[0]
    for step in range(1, rows):
        both = both + stats[step]
    mean = both[:, 0:1] / D
    var = jnp.maximum(both[:, 64:65] / D - mean * mean, 0.0)
    mine[...] = ((xf - mean) * lax.rsqrt(var + EPS) * gain_ref[...]).astype(jnp.bfloat16)
    place = pl.ds(pl.multiple_of(me_col * patches, patches), patches)
    keep = pltpu.make_async_copy(mine, out_ref.at[place], local_sem)
    keep.start()
    copies = []
    for step in range(1, cols):
        copy = pltpu.make_async_remote_copy(
            src_ref=mine,
            dst_ref=out_ref.at[place],
            send_sem=send.at[step],
            recv_sem=recv.at[step],
            device_id={"col": lax.rem(me_col + step, cols)},
            device_id_type=MESH,
        )
        copy.start()
        copies.append(copy)
    for copy in copies:
        copy.wait()
    keep.wait()


def norm_gather(x, gain, rows, cols):
    patches, width = x.shape
    return pl.pallas_call(
        functools.partial(norm_kernel, rows, cols),
        out_shape=jax.ShapeDtypeStruct((patches * cols, width), jnp.bfloat16),
        in_specs=[vmem(), vmem()],
        out_specs=vmem(),
        scratch_shapes=[
            pltpu.VMEM((patches, width), jnp.bfloat16),
            pltpu.VMEM((rows, patches, 128), jnp.float32),
            pltpu.SemaphoreType.DMA((rows,)),
            pltpu.SemaphoreType.DMA((rows,)),
            pltpu.SemaphoreType.DMA((cols,)),
            pltpu.SemaphoreType.DMA((cols,)),
            pltpu.SemaphoreType.DMA,
        ],
        compiler_params=params(0),
    )(x, gain)


def reduce_kernel(rows, q_ref, k_ref, v_ref, m_ref, out_ref, low, high, low_send, low_recv, high_send, high_recv):
    me = lax.axis_index("row")
    last = rows - 1
    pieces = q_ref.shape[0] // PIECE
    greet_line(me, rows)

    def copy_of(held, send, recv, p, target):
        place = pl.ds(pl.multiple_of(p * PIECE, PIECE), PIECE)
        return pltpu.make_async_remote_copy(
            src_ref=held.at[place],
            dst_ref=held.at[place],
            send_sem=send.at[p],
            recv_sem=recv.at[p],
            device_id={"row": target},
            device_id_type=MESH,
        )

    def low_copy(p):
        return copy_of(low, low_send, low_recv, p, jnp.maximum(me - 1, 0))

    def high_copy(p):
        return copy_of(high, high_send, high_recv, p, jnp.minimum(me + 1, last))

    def add(held, p, side, is_source, is_sink):
        place = pl.ds(pl.multiple_of(p * PIECE, PIECE), PIECE)
        offset = 0
        for ref in (q_ref, k_ref, v_ref, m_ref):
            half = ref.shape[1] // 2
            mine = ref[place, side * half : (side + 1) * half]
            columns = slice(offset, offset + half)
            offset += half

            @pl.when(is_source)
            def _():
                held[place, columns] = mine

            @pl.when(jnp.logical_not(is_source))
            def _():
                total = mine.astype(jnp.float32) + held[place, columns].astype(jnp.float32)

                @pl.when(is_sink)
                def _():
                    out_ref[place, columns] = total.astype(jnp.bfloat16)

                @pl.when(jnp.logical_not(is_sink))
                def _():
                    held[place, columns] = total.astype(jnp.bfloat16)

    def step(s, carry):
        p_low = s - SKEW * (last - me)
        p_high = s - SKEW * me
        low_on = jnp.logical_and(p_low >= 0, p_low < pieces)
        high_on = jnp.logical_and(p_high >= 0, p_high < pieces)

        @pl.when(low_on)
        def _():
            @pl.when(me < last)
            def _():
                low_copy(p_low).wait_recv()

            add(low, p_low, 0, me == last, me == 0)

        @pl.when(high_on)
        def _():
            @pl.when(me > 0)
            def _():
                high_copy(p_high).wait_recv()

            add(high, p_high, 1, me == 0, me == last)

        @pl.when(jnp.logical_and(low_on, me > 0))
        def _():
            low_copy(p_low).start()

        @pl.when(jnp.logical_and(high_on, me < last))
        def _():
            high_copy(p_high).start()

        return carry

    lax.fori_loop(0, pieces + SKEW * last, step, 0)

    def drain(p, carry):
        @pl.when(me > 0)
        def _():
            low_copy(p).wait_send()

        @pl.when(me < last)
        def _():
            high_copy(p).wait_send()

        return carry

    lax.fori_loop(0, pieces, drain, 0)


def reduce_line(parts, rows):
    patches = parts[0].shape[0]
    width = sum(part.shape[1] for part in parts) // 2
    pieces = patches // PIECE
    return pl.pallas_call(
        functools.partial(reduce_kernel, rows),
        out_shape=jax.ShapeDtypeStruct((patches, width), jnp.bfloat16),
        in_specs=[vmem()] * len(parts),
        out_specs=vmem(),
        scratch_shapes=[
            pltpu.VMEM((patches, width), jnp.bfloat16),
            pltpu.VMEM((patches, width), jnp.bfloat16),
        ]
        + [pltpu.SemaphoreType.DMA((pieces,))] * 4,
        compiler_params=params(1),
    )(*parts)


def spread_kernel(rows, attn_ref, act_ref, attn_out, act_out, sems, local_sem):
    me = lax.axis_index("row")
    last = rows - 1
    pieces = attn_ref.shape[0] // PIECE
    greet_line(me, rows)
    pairs = ((attn_ref, attn_out), (act_ref, act_out))

    def piece_of(ref, p, side):
        half = ref.shape[1] // 2
        return ref.at[pl.ds(pl.multiple_of(p * PIECE, PIECE), PIECE), pl.ds(side * half, half)]

    def copies(p, side, own, target):
        out = []
        for index, (source, full) in enumerate(pairs):
            place = piece_of(full, p, side)
            src = source.at[pl.ds(pl.multiple_of(p * PIECE, PIECE), PIECE)] if own else place
            out.append(
                pltpu.make_async_remote_copy(
                    src_ref=src,
                    dst_ref=place,
                    send_sem=sems.at[0, side, index, p],
                    recv_sem=sems.at[1, side, index, p],
                    device_id={"row": target},
                    device_id_type=MESH,
                )
            )
        return out

    up, down = jnp.minimum(me + 1, last), jnp.maximum(me - 1, 0)

    for side, owner, target in ((0, 0, up), (1, last, down)):

        @pl.when(me == owner)
        def _():
            for index, (source, full) in enumerate(pairs):
                half = full.shape[1] // 2
                pltpu.make_async_copy(
                    source, full.at[:, pl.ds(side * half, half)], local_sem.at[index]
                ).start()

            def push(p, carry):
                for copy in copies(p, side, True, target):
                    copy.start()
                return carry

            lax.fori_loop(0, pieces, push, 0)

    def step(s, carry):
        for side, hops, target, end in ((0, me, up, last), (1, last - me, down, 0)):
            p = s - SKEW * hops

            @pl.when(jnp.logical_and(hops > 0, jnp.logical_and(p >= 0, p < pieces)))
            def _():
                moved = copies(p, side, False, target)
                for copy in moved:
                    copy.wait_recv()

                @pl.when(me != end)
                def _():
                    for copy in moved:
                        copy.start()

        return carry

    lax.fori_loop(0, pieces + SKEW * last, step, 0)

    def drain(p, carry):
        for side, target, end in ((0, up, last), (1, down, 0)):

            @pl.when(me != end)
            def _():
                for copy in copies(p, side, False, target):
                    copy.wait_send()

        return carry

    lax.fori_loop(0, pieces, drain, 0)
    for side, owner in ((0, 0), (1, last)):

        @pl.when(me == owner)
        def _():
            for index, (source, full) in enumerate(pairs):
                half = full.shape[1] // 2
                pltpu.make_async_copy(
                    source, full.at[:, pl.ds(side * half, half)], local_sem.at[index]
                ).wait()


def spread_line(attn, act, rows):
    patches = attn.shape[0]
    pieces = patches // PIECE
    return pl.pallas_call(
        functools.partial(spread_kernel, rows),
        out_shape=[
            jax.ShapeDtypeStruct((patches, 2 * value.shape[1]), value.dtype) for value in (attn, act)
        ],
        in_specs=[vmem(), vmem()],
        out_specs=[vmem(), vmem()],
        scratch_shapes=[
            pltpu.SemaphoreType.DMA((2, 2, 2, pieces)),
            pltpu.SemaphoreType.DMA((2,)),
        ],
        compiler_params=params(2),
    )(attn, act)


def finish_kernel(cols, part_ref, x_ref, out_ref, held, send, recv):
    me = lax.axis_index("col")
    patches = x_ref.shape[0]
    greet_peers((("col", cols),))

    def block(owner):
        return pl.ds(pl.multiple_of(owner * patches, patches), patches)

    copies = []
    for step in range(1, cols):
        peer = lax.rem(me + step, cols)
        copy = pltpu.make_async_remote_copy(
            src_ref=part_ref.at[block(peer)],
            dst_ref=held.at[step - 1],
            send_sem=send.at[step],
            recv_sem=recv.at[step],
            device_id={"col": peer},
            device_id_type=MESH,
        )
        copy.start()
        copies.append(copy)
    total = part_ref[block(me)].astype(jnp.float32)
    for copy in copies:
        copy.wait()
    for step in range(1, cols):
        total = total + held[step - 1].astype(jnp.float32)
    out_ref[...] = (x_ref[...].astype(jnp.float32) + total).astype(jnp.bfloat16)


def finish(part, x, cols):
    patches, width = x.shape
    return pl.pallas_call(
        functools.partial(finish_kernel, cols),
        out_shape=jax.ShapeDtypeStruct((patches, width), jnp.bfloat16),
        in_specs=[vmem(), vmem()],
        out_specs=vmem(),
        scratch_shapes=[
            pltpu.VMEM((cols - 1, patches, width), jnp.bfloat16),
            pltpu.SemaphoreType.DMA((cols,)),
            pltpu.SemaphoreType.DMA((cols,)),
        ],
        compiler_params=params(3),
    )(part, x)


def line_layer(x, weights):
    gain, wq, wk, wv, wup, wout, wdown = weights
    rows, cols = lax.axis_size("row"), lax.axis_size("col")
    here = x[0]
    gathered = norm_gather(here, gain[None], rows, cols)
    parts = [
        jnp.dot(gathered, w, preferred_element_type=jnp.float32).astype(jnp.bfloat16)
        for w in (wq, wk, wv, wup)
    ]
    summed = reduce_line(parts, rows)
    head_dim = D // HEADS
    width = wq.shape[1] // 2
    heads = width // head_dim
    query, keyed, valued = (
        summed[:, i * width : (i + 1) * width].reshape(-1, heads, head_dim) for i in range(3)
    )
    pre = summed[:, 3 * width :].astype(jnp.float32)
    act = jax.nn.gelu(pre, approximate=False).astype(jnp.bfloat16)
    scores = jnp.einsum("qhd,khd->hqk", query, keyed, preferred_element_type=jnp.float32) / jnp.sqrt(
        jnp.float32(head_dim)
    )
    scores = scores - jnp.max(scores, axis=-1, keepdims=True)
    expo = jnp.exp(scores)
    probs = (expo / jnp.sum(expo, axis=-1, keepdims=True)).astype(jnp.bfloat16)
    attn = jnp.einsum("hqk,khd->qhd", probs, valued, preferred_element_type=jnp.float32)
    attn = attn.reshape(-1, width).astype(jnp.bfloat16)
    attn_full, act_full = spread_line(attn, act, rows)
    mixed = jnp.dot(attn_full, wout, preferred_element_type=jnp.float32) + jnp.dot(
        act_full, wdown, preferred_element_type=jnp.float32
    )
    return finish(mixed.astype(jnp.bfloat16), here, cols)[None]


def halves(x, wq, wup):
    patches = x.shape[1]
    return (
        lax.axis_size("row") > 1
        and lax.axis_size("col") > 1
        and patches % PIECE == 0
        and (wq.shape[1] // 2) % (D // HEADS) == 0
        and (wup.shape[1] // 2) % 128 == 0
    )


def passed_along(value, axis, steps):
    count = lax.axis_size(axis)
    first, last = (max(0, -steps), min(count, count - steps))
    return lax.ppermute(value, axis, [(source, source + steps) for source in range(first, last)])


def layer(x, weights):
    gain, wq, wk, wv, wup, wout, wdown = weights
    xf = x.astype(jnp.float32)
    sums, squares = lax.psum((jnp.sum(xf, axis=-1), jnp.sum(xf * xf, axis=-1)), "row")
    mean = (sums / D)[..., None]
    var = jnp.maximum((squares / D)[..., None] - mean * mean, 0.0)
    normed = ((xf - mean) * lax.rsqrt(var + EPS) * gain).astype(jnp.bfloat16)
    gathered = lax.all_gather(normed, "col", axis=1, tiled=True)
    part_q = jnp.dot(gathered, wq, preferred_element_type=jnp.float32)
    part_k = jnp.dot(gathered, wk, preferred_element_type=jnp.float32)
    part_v = jnp.dot(gathered, wv, preferred_element_type=jnp.float32)
    part_m = jnp.dot(gathered, wup, preferred_element_type=jnp.float32)
    query, keyed, valued, pre = (
        lax.psum_scatter(
            part_q.astype(jnp.bfloat16), "row", scatter_dimension=1, tiled=True
        ).astype(jnp.float32),
        lax.psum_scatter(
            part_k.astype(jnp.bfloat16), "row", scatter_dimension=1, tiled=True
        ).astype(jnp.float32),
        lax.psum_scatter(
            part_v.astype(jnp.bfloat16), "row", scatter_dimension=1, tiled=True
        ).astype(jnp.float32),
        lax.psum_scatter(
            part_m.astype(jnp.bfloat16), "row", scatter_dimension=1, tiled=True
        ).astype(jnp.float32),
    )
    act = jax.nn.gelu(pre, approximate=False).astype(jnp.bfloat16)
    query = query.astype(jnp.bfloat16)
    keyed = keyed.astype(jnp.bfloat16)
    valued = valued.astype(jnp.bfloat16)
    all_keys, all_values = (
        lax.all_gather(keyed, "row", axis=1, tiled=True),
        lax.all_gather(valued, "row", axis=1, tiled=True),
    )
    head_dim = D // HEADS
    local_heads = query.shape[2] // head_dim
    images = query.shape[0]
    qh = query.reshape(images, query.shape[1], local_heads, head_dim)
    kh = all_keys.reshape(images, all_keys.shape[1], local_heads, head_dim)
    vh = all_values.reshape(images, all_values.shape[1], local_heads, head_dim)
    scores = jnp.einsum("bqhd,bkhd->bhqk", qh, kh, preferred_element_type=jnp.float32) / jnp.sqrt(
        jnp.float32(head_dim)
    )
    scores = scores - jnp.max(scores, axis=-1, keepdims=True)
    expo = jnp.exp(scores)
    probs = (expo / jnp.sum(expo, axis=-1, keepdims=True)).astype(jnp.bfloat16)
    attn = jnp.einsum("bhqk,bkhd->bqhd", probs, vh, preferred_element_type=jnp.float32)
    attn = attn.reshape(query.shape).astype(jnp.bfloat16)
    attn_full, act_full = (
        lax.all_gather(attn, "row", axis=1, tiled=True),
        lax.all_gather(act, "row", axis=1, tiled=True),
    )
    mixed = jnp.dot(attn_full, wout, preferred_element_type=jnp.float32) + jnp.dot(
        act_full, wdown, preferred_element_type=jnp.float32
    )
    summed = lax.psum_scatter(
        mixed.astype(jnp.bfloat16), "col", scatter_dimension=1, tiled=True
    ).astype(jnp.float32)
    return (xf + summed).astype(jnp.bfloat16)


def pass_on(output):
    return passed_along(output, "section", 1)


def local(tokens, ln_gain, w_query, w_key, w_value, w_up, w_out, w_down):
    weights = (ln_gain[0], w_query[0], w_key[0], w_value[0], w_up[0], w_out[0], w_down[0])
    section = lax.axis_index("section")
    sections = lax.axis_size("section")
    result = jnp.zeros_like(tokens)
    images = tokens.shape[0]
    ticks = images + sections - 1
    inbox = jnp.zeros_like(tokens[:1])
    positions = jnp.arange(images, dtype=jnp.int32)
    step = line_layer if halves(tokens, w_query[0], w_up[0]) else layer
    for tick in range(ticks):
        fresh = tokens[min(tick, images - 1) : min(tick, images - 1) + 1]
        current = jnp.where(section == 0, fresh, inbox)
        output = step(current, weights)
        slot = tick - section
        result = jnp.where((positions == slot)[:, None, None], output, result)
        if tick + 1 < ticks:
            inbox = pass_on(output)
    return result[None]


def solution(mesh):
    return jax.shard_map(
        local,
        mesh=mesh,
        in_specs=(
            P(None, "col", "row"),
            P("section", "row"),
            P("section", "row", "col"),
            P("section", "row", "col"),
            P("section", "row", "col"),
            P("section", "row", "col"),
            P("section", "col", "row"),
            P("section", "col", "row"),
        ),
        out_specs=P("section", None, "col", "row"),
        check_vma=False,
    )
```
